512 devices in a mesh: groups: 2 (over y), seq: 16 (over z), heads: 8 (over x), sub: 2 (over core).
Axes of the slice: x: 8, y: 2, z: 16, core: 2. Of those that a mesh axis runs over, the one named last changes fastest.
The devices are a block of a 8x8x16 slice.
Arguments:
- queries: bfloat16 [8192, 8192], P(('groups', 'seq', 'sub'), 'heads'), parts along dimension 0, may hold values from -400 to 400
- keys: bfloat16 [8192, 1024], P(('groups', 'seq', 'sub'), 'heads'), parts along dimension 0, may hold values from -6 to 6
- values: bfloat16 [8192, 1024], P(('groups', 'seq', 'sub'), 'heads'), parts along dimension 0, may hold values from -18 to 18
- half_order: int32 [128], P('groups'), parts along dimension 0, may hold values from 0 to 63, as said below
- frame_lengths: int32 [64], P('groups'), parts along dimension 0, may hold values from 1 to 256, 4096 in all
- out_proj: bfloat16 [8192, 4096], P('heads', ('seq', 'sub')), may hold values from -0.125 to 0.125
- residual_in: bfloat16 [8192, 4096], P(('groups', 'seq', 'sub'), 'heads'), parts along dimension 0, may hold values from -40 to 40
- norm_gain: float32 [4096], P('heads'), may hold values from 0.5 to 1.5
Outputs:
- attended: bfloat16 [8192, 8192], P(('groups', 'seq', 'sub'), 'heads'), parts along dimension 0
- hidden_state: bfloat16 [8192, 4096], P(('groups', 'seq', 'sub'), 'heads'), parts along dimension 0
- normed: bfloat16 [8192, 4096], P(('groups', 'seq', 'sub'), 'heads'), parts along dimension 0
The draws below stay inside these ranges and needn't reach their ends.
There are 2 independent parts, one for each index of `groups`. The reference program is written for one: setup_inputs(seed, part) draws one part's arguments, and reference() takes and returns one part's arrays. A program takes and returns all parts, laid end to end along the dimension named above; an argument that names none is the same for every part. Nothing has to cross between parts.
Inputs may be any that keep to these rules, and one draw needn't show every extreme that they name: `half_order`: a permutation of 0 to 63.
All inputs are finite; a program needn't handle non-finite values.
Results may differ from the reference program's by a relative error of at most 0.005.
Values may be sent and summed in bfloat16 or wider, within the bound.
No kernel may reach another device: no remote copies, remote signals or barrier semaphores. Data moves between devices by JAX's collectives and lax.ppermute only.
A program may use at most 64 MiB of HBM per device.

```python
import math
import jax
import jax.numpy as jnp
import numpy as np
from jax import lax

QUERY_HEAD_COUNT = 64
KEY_VALUE_HEADS = 8
HEAD_WIDTH = 128
OUT_WIDTH = 4096
CLIP_TOKENS = 4096
HALF = 64
HALVES = 64
FRAMES = 32
FRAME_MOST = 256


def order_table(key):
    return jax.random.permutation(jax.random.fold_in(key, 11), HALVES).astype(jnp.int32)


def draw_half_order(key, part):
    return order_table(key)


def draw_keys(key, part):
    filled_rows = jax.random.normal(jax.random.fold_in(key, 17), (CLIP_TOKENS, KEY_VALUE_HEADS * HEAD_WIDTH), jnp.float32)
    return jnp.clip(filled_rows, -6.0, 6.0).astype(jnp.bfloat16)


def draw_queries(key, part):
    filled_rows = 1.5 * jax.random.normal(jax.random.fold_in(key, 31), (CLIP_TOKENS, QUERY_HEAD_COUNT * HEAD_WIDTH), jnp.float32)
    return jnp.clip(filled_rows, -400.0, 400.0).astype(jnp.bfloat16)


def draw_residual_in(key, part):
    column_base = jnp.exp(math.log(4.0) * jnp.arange(OUT_WIDTH, dtype=jnp.float32) / OUT_WIDTH) * 0.5
    column_jitter = jnp.exp(jax.random.uniform(jax.random.fold_in(key, 41), (OUT_WIDTH,), jnp.float32, math.log(0.7), math.log(1.4)))
    entries = jax.random.normal(jax.random.fold_in(key, 43), (CLIP_TOKENS, OUT_WIDTH), jnp.float32)
    row_scale = jnp.exp(jax.random.uniform(jax.random.fold_in(key, 47), (CLIP_TOKENS,), jnp.float32, 0.0, math.log(10.0)))
    filled_rows = entries * (column_base * column_jitter)[None, :] * row_scale[:, None]
    return jnp.clip(filled_rows, -40.0, 40.0).astype(jnp.bfloat16)


def strengthened(values, key, source, target, parts, factor):
    owner, partner = [(jnp.arange(values.shape[dim]) // (values.shape[dim] // parts)).reshape([-1 if axis == dim else 1 for axis in range(values.ndim)]) for dim in (source, target)]
    chosen = jax.random.permutation(key, parts)[partner]
    strong = (owner == chosen) | (owner == (partner + parts // 2) % parts)
    return jnp.where(strong, factor * values, values)


def block_scale(stream_key, shape, split, least, top_value):
    loudness, own = 1.0, jax.random.fold_in(stream_key, 6)
    for dim, parts in split:
        draws = jnp.exp(jax.random.uniform(jax.random.fold_in(own, dim), (parts,), jnp.float32, least / len(split), top_value / len(split)))
        loudness = loudness * jnp.repeat(draws, shape[dim] // parts).reshape([-1 if axis == dim else 1 for axis in range(len(shape))])
    return loudness


def profile(count, total, most, skew):
    loads = [(1 << 20) // math.isqrt(grade ** skew) + 1 for grade in range(2, count + 1)]
    spare, counts = total - most - (count - 1), [1] * (count - 1)
    while spare > 0:
        free = [i for i in range(count - 1) if counts[i] < most]
        whole, budget = sum([loads[i] for i in free]), spare
        for i in free:
            more = min(most - counts[i], max(1, budget * loads[i] // whole), spare)
            counts[i] = counts[i] + more
            spare = spare - more
    return np.array([most] + counts)


def ragged(own_key, count, total, reach, slope):
    if count == 2:
        one = jax.random.randint(own_key, (), max(1, total - reach), min(reach, total - 1) + 1)
        return jnp.stack([one, total - one])
    sizes = jnp.asarray(profile(count, total, reach, slope), jnp.int32)
    couples = (count - 1) // 2
    source_of, taker = sizes[1:1 + 2 * couples:2], sizes[2:2 + 2 * couples:2]
    slack = jnp.minimum(source_of - 1, reach - taker)
    passed = jax.random.randint(jax.random.fold_in(own_key, 1), (couples,), 0, 1 << 20) % (slack + 1)
    sizes = sizes.at[1:1 + 2 * couples:2].set(source_of - passed).at[2:2 + 2 * couples:2].set(taker + passed)
    return sizes[jax.random.permutation(jax.random.fold_in(own_key, 2), count)]


def normal_values(key, shape, scale, limit, pieces=(), held_as=jnp.bfloat16):
    gain = block_scale(key, shape, pieces, -0.22, 0.18) if pieces else 1.0
    array = jax.random.normal(key, shape, jnp.float32) * scale * gain
    return jnp.minimum(jnp.maximum(array, -limit), limit).astype(held_as)


def gaussian_with(own_key, extent, deviation, most, cuts, heavy, held_as=jnp.bfloat16):
    array = deviation * jax.random.normal(own_key, extent, jnp.float32)
    if cuts:
        array = array * block_scale(own_key, extent, cuts, -0.22, 0.18)
    return jnp.clip(strengthened(array, jax.random.fold_in(own_key, 3), *heavy), -most, most).astype(held_as)


def setup_inputs(seed: int = 0, part: int = 0) -> dict:
    arg_keys = jax.random.split(jax.random.key(seed), 9)
    part_keys = jax.random.split(jax.random.fold_in(arg_keys[8], part), 9)
    queries = draw_queries(jax.random.fold_in(jax.random.fold_in(arg_keys[8], part), 71), part)
    keys = draw_keys(jax.random.fold_in(jax.random.fold_in(arg_keys[8], part), 71), part)
    values = normal_values(part_keys[2], (CLIP_TOKENS, KEY_VALUE_HEADS * HEAD_WIDTH), 3.0, 18.0, ((0, 32), (1, 8)))
    half_order = draw_half_order(jax.random.fold_in(jax.random.fold_in(arg_keys[8], part), 71), part)
    frame_lengths = ragged(part_keys[4], FRAMES, CLIP_TOKENS, FRAME_MOST, 2).astype(jnp.int32)
    out_proj = gaussian_with(arg_keys[5], (QUERY_HEAD_COUNT * HEAD_WIDTH, OUT_WIDTH), (QUERY_HEAD_COUNT * HEAD_WIDTH) ** -0.5, 0.125, ((0, 8), (1, 32)), (0, 1, 32, 2.75))
    residual_in = draw_residual_in(jax.random.fold_in(jax.random.fold_in(arg_keys[8], part), 71), part)
    norm_gain = jnp.clip(1.0 + 0.1 * jax.random.normal(arg_keys[7], (OUT_WIDTH,), jnp.float32), 0.5, 1.5)
    return dict(queries=queries, keys=keys, values=values, half_order=half_order, frame_lengths=frame_lengths, out_proj=out_proj, residual_in=residual_in, norm_gain=norm_gain)


def positions_of(half_order):
    row_ids = jnp.arange(CLIP_TOKENS, dtype=jnp.int32)
    return (half_order[row_ids // HALF] * HALF + row_ids % HALF).astype(jnp.int32)

def frame_limits(position, frame_lengths):
    frame_ends = jnp.cumsum(frame_lengths).astype(jnp.int32)
    frame_starts = frame_ends - frame_lengths
    chosen = jnp.where(frame_starts[None, :] <= position[:, None], frame_lengths[None, :], 0)
    return lax.optimization_barrier(jnp.sum(chosen, axis=1)).astype(jnp.int32)

def reference(queries, keys, values, half_order, frame_lengths, out_proj, residual_in, norm_gain):
    group_width = QUERY_HEAD_COUNT // KEY_VALUE_HEADS
    position = positions_of(half_order)
    frame_end = frame_limits(position, frame_lengths)
    query_head_rows = queries.reshape(CLIP_TOKENS, KEY_VALUE_HEADS, group_width, HEAD_WIDTH)
    key_head_rows = keys.reshape(CLIP_TOKENS, KEY_VALUE_HEADS, HEAD_WIDTH)
    value_head_rows = values.reshape(CLIP_TOKENS, KEY_VALUE_HEADS, HEAD_WIDTH)
    block_rows = min(512, CLIP_TOKENS)
    block_count = CLIP_TOKENS // block_rows

    def single_head(kv_head):
        key_one = key_head_rows[:, kv_head].astype(jnp.float32)
        value_one = value_head_rows[:, kv_head].astype(jnp.float32)
        query_one = query_head_rows[:, kv_head]

        def one_block(block_id):
            query_block = lax.dynamic_slice_in_dim(query_one, block_id * block_rows, block_rows, 0).astype(jnp.float32)
            limit_block = lax.dynamic_slice_in_dim(frame_end, block_id * block_rows, block_rows, 0)
            scores = jnp.einsum('qgd,kd->gqk', query_block, key_one) * HEAD_WIDTH ** (-0.5)
            visible = position[None, :] < limit_block[:, None]
            scores = jnp.where(visible[None], scores, -1e+30)
            row_max = lax.optimization_barrier(jnp.max(scores, axis=-1, keepdims=True))
            weights = jnp.where(visible[None], jnp.exp(scores - row_max), 0.0)
            total = lax.optimization_barrier(jnp.sum(weights, axis=-1))
            rounded = weights.astype(jnp.bfloat16).astype(jnp.float32)
            summed = jnp.einsum('gqk,kd->qgd', rounded, value_one)
            return (summed / jnp.transpose(total)[:, :, None]).astype(jnp.bfloat16)
        blocks = lax.map(one_block, jnp.arange(block_count, dtype=jnp.int32))
        return blocks.reshape(CLIP_TOKENS, group_width, HEAD_WIDTH)
    each_head_rows = lax.map(single_head, jnp.arange(KEY_VALUE_HEADS, dtype=jnp.int32))
    attended = jnp.transpose(each_head_rows, (1, 0, 2, 3)).reshape(CLIP_TOKENS, QUERY_HEAD_COUNT * HEAD_WIDTH)
    projected = jnp.dot(attended, out_proj, preferred_element_type=jnp.float32)
    hidden_state = (residual_in.astype(jnp.float32) + projected).astype(jnp.bfloat16)
    widened = hidden_state.astype(jnp.float32)
    energy = lax.optimization_barrier(jnp.sum(widened * widened, axis=-1)) / OUT_WIDTH
    normed = (widened * lax.rsqrt(energy + 1e-06)[:, None] * norm_gain.astype(jnp.float32)[None, :]).astype(jnp.bfloat16)
    return (attended, hidden_state, normed)
```

```python
import jax
import jax.numpy as jnp
from jax import lax
from jax.experimental import pallas as pl
from jax.experimental.pallas import tpu as pltpu
from jax.sharding import PartitionSpec as P

HEAD_WIDTH = 128
SCALE = HEAD_WIDTH ** (-0.5)


def swapped(value):
    return lax.ppermute(value, "sub", [(0, 1), (1, 0)])


def everyone_sum(value):
    copies = jnp.broadcast_to(value, (lax.axis_size("heads"), *value.shape))
    return lax.all_to_all(copies, "heads", split_axis=0, concat_axis=0, tiled=True).sum(axis=0)


def attend_kernel(q_ref, k_ref, v_ref, kv_ref, pos_ref, limit_ref, out_ref):
    own = k_ref.shape[0]
    keys = (k_ref[...], kv_ref[:own])
    values = (v_ref[...], kv_ref[own:])
    scores = []
    for j in range(2):
        part = lax.dot_general(
            q_ref[...], keys[j], (((1,), (1,)), ((), ())), preferred_element_type=jnp.float32
        )
        visible = pos_ref[:, j * own : (j + 1) * own] < limit_ref[...]
        scores.append(jnp.where(visible, part * SCALE, -1e30))
    row_max = jnp.maximum(
        jnp.max(scores[0], axis=-1, keepdims=True), jnp.max(scores[1], axis=-1, keepdims=True)
    )
    total, product = 0.0, 0.0
    for j in range(2):
        weights = jnp.exp(scores[j] - row_max)
        total += jnp.sum(weights, axis=-1, keepdims=True)
        product += jnp.dot(
            weights.astype(jnp.bfloat16), values[j], preferred_element_type=jnp.float32
        )
    out_ref[...] = (product / total).astype(out_ref.dtype)


def attend(queries, keys, values, kv_other, key_pos, limit):
    rows, width = queries.shape
    heads, count = width // HEAD_WIDTH, key_pos.shape[1]
    whole = lambda a: pl.BlockSpec(a.shape, lambda h: (0, 0))
    return pl.pallas_call(
        attend_kernel,
        grid=(heads,),
        in_specs=[
            pl.BlockSpec((rows, HEAD_WIDTH), lambda h: (0, h)),
            whole(keys),
            whole(values),
            whole(kv_other),
            whole(key_pos),
            whole(limit),
        ],
        out_specs=pl.BlockSpec((rows, HEAD_WIDTH), lambda h: (0, h)),
        out_shape=jax.ShapeDtypeStruct((rows, width), jnp.bfloat16),
        compiler_params=pltpu.CompilerParams(vmem_limit_bytes=24 << 20),
        cost_estimate=pl.CostEstimate(
            flops=4 * rows * width * count,
            bytes_accessed=4 * rows * width + 4 * count * HEAD_WIDTH,
            transcendentals=rows * heads * count,
        ),
    )(queries, keys, values, kv_other, key_pos, limit)


def project_kernel(a_ref, w_ref, out_ref):
    rows = out_ref.shape[2]
    wide = w_ref.shape[2]
    for j in range(w_ref.shape[0]):
        part = jnp.dot(a_ref[...], w_ref[j], preferred_element_type=jnp.float32)
        part = part.astype(jnp.bfloat16)
        for c in range(out_ref.shape[1]):
            out_ref[0, c, :, j * wide : (j + 1) * wide] = part[c * rows : (c + 1) * rows]


def project(both, weights, nx):
    chips, depth, wide = weights.shape
    rows, per = both.shape[0] // 2, chips // nx
    return pl.pallas_call(
        project_kernel,
        grid=(nx,),
        in_specs=[
            pl.BlockSpec(both.shape, lambda h: (0, 0)),
            pl.BlockSpec((per, depth, wide), lambda h: (h, 0, 0)),
        ],
        out_specs=pl.BlockSpec((1, 2, rows, per * wide), lambda h: (h, 0, 0, 0)),
        out_shape=jax.ShapeDtypeStruct((nx, 2, rows, per * wide), jnp.bfloat16),
        compiler_params=pltpu.CompilerParams(vmem_limit_bytes=16 << 20),
        cost_estimate=pl.CostEstimate(
            flops=4 * rows * depth * wide * chips,
            bytes_accessed=2 * weights.size,
            transcendentals=0,
        ),
    )(both, weights)


def shards(queries, keys, values, half_order, frame_lengths, out_proj, residual_in, norm_gain):
    tok_rows = queries.shape[0]
    half_rows = tok_rows // 2
    chips, nx = lax.axis_size("seq"), lax.axis_size("heads")
    z, core = lax.axis_index("seq"), lax.axis_index("sub")
    features = residual_in.shape[1] * nx

    weights = lax.all_gather(out_proj, "seq")
    k_own = lax.all_gather(keys, "seq", tiled=True)
    v_own = lax.all_gather(values, "seq", tiled=True)
    kv_other = swapped(jnp.concatenate([k_own, v_own], axis=0))

    inner = jnp.arange(half_rows, dtype=jnp.int32)
    table = (half_order[:, None] * half_rows + inner[None, :]).reshape(chips, 2, tok_rows)
    of_core = [table[:, 0].reshape(1, -1), table[:, 1].reshape(1, -1)]
    key_pos = jnp.where(
        core == 0,
        jnp.concatenate(of_core, axis=1),
        jnp.concatenate(of_core[::-1], axis=1),
    )
    chosen = (jnp.arange(2 * chips, dtype=jnp.int32) == 2 * z + core)[:, None]
    query_pos = jnp.sum(jnp.where(chosen, table.reshape(2 * chips, tok_rows), 0), axis=0)
    frame_starts = jnp.cumsum(frame_lengths) - frame_lengths
    limit = jnp.sum(
        jnp.where(frame_starts[None, :] <= query_pos[:, None], frame_lengths[None, :], 0), axis=1
    )[:, None]
    attended = attend(queries, k_own, v_own, kv_other, key_pos, limit)

    both = lax.all_gather(attended, "sub", tiled=True)
    parts = project(both, weights, nx)
    per = chips // nx
    parts = parts.reshape(2 * nx, tok_rows, -1)
    parts = lax.all_to_all(parts, ("heads", "sub"), 0, 0, tiled=True)
    parts = parts.reshape(nx, 2, tok_rows, per, -1)
    projected = jnp.sum(parts.astype(jnp.float32), axis=0)
    projected = jnp.transpose(projected, (1, 2, 0, 3)).reshape(tok_rows, -1)

    hidden_state = (residual_in.astype(jnp.float32) + projected).astype(jnp.bfloat16)
    widened = hidden_state.astype(jnp.float32)
    energy = everyone_sum(jnp.sum(widened * widened, axis=1)) / features
    normed = (widened * lax.rsqrt(energy + 1e-06)[:, None] * norm_gain[None, :]).astype(
        jnp.bfloat16
    )
    return (attended, hidden_state, normed)


def solution(mesh):
    rows = P(("groups", "seq", "sub"), "heads")
    in_specs = (rows, rows, rows, P("groups"), P("groups"), P("heads", ("seq", "sub")), rows, P("heads"))
    return jax.shard_map(
        shards, mesh=mesh, in_specs=in_specs, out_specs=(rows, rows, rows), check_vma=False
    )
```

```python
import functools
import math

import jax
import jax.numpy as jnp
from jax import lax
from jax.experimental import pallas as pl
from jax.experimental.pallas import tpu as pltpu
from jax.sharding import PartitionSpec as P

HEAD_WIDTH = 128
EXP_SCALE = HEAD_WIDTH ** (-0.5) * math.log2(math.e)
VMEM = pl.BlockSpec(memory_space=pltpu.VMEM)


def swapped(value):
    return lax.ppermute(value, "sub", [(0, 1), (1, 0)])


def attend_kernel(q_ref, k_ref, v_ref, kv_ref, pos_ref, limit_ref, out_ref, bias_ref):
    own, rows = k_ref.shape[0], q_ref.shape[0]
    keys = own // 4

    @pl.when(pl.program_id(0) == 0)
    def _():
        bias_ref[...] = jnp.where(pos_ref[...] < limit_ref[...], 0.0, -1e30)

    q = jnp.concatenate([q_ref[:, :HEAD_WIDTH], q_ref[:, HEAD_WIDTH:]], axis=0)
    scores = []
    for j in range(8):
        ref, at = (k_ref, j * keys) if j < 4 else (kv_ref, (j - 4) * keys)
        part = lax.dot_general(
            q, ref[at : at + keys], (((1,), (1,)), ((), ())), preferred_element_type=jnp.float32
        )
        bias = bias_ref[:, j * keys : (j + 1) * keys]
        scores.append(jnp.concatenate([part[:rows] + bias, part[rows:] + bias], axis=0))
    row_max = scores[0]
    for part in scores[1:]:
        row_max = jnp.maximum(row_max, part)
    row_max = jnp.max(row_max, axis=-1, keepdims=True) * EXP_SCALE
    total, product = 0.0, 0.0
    for j in range(8):
        ref, at = (v_ref, j * keys) if j < 4 else (kv_ref, own + (j - 4) * keys)
        weights = jnp.exp2(scores[j] * EXP_SCALE - row_max)
        total += weights
        product += jnp.dot(
            weights.astype(jnp.bfloat16), ref[at : at + keys], preferred_element_type=jnp.float32
        )
    result = (product / jnp.sum(total, axis=-1, keepdims=True)).astype(out_ref.dtype)
    out_ref[:, :HEAD_WIDTH] = result[:rows]
    out_ref[:, HEAD_WIDTH:] = result[rows:]


def attend(queries, keys, values, kv_other, key_pos, limit):
    rows, width = queries.shape
    heads, count = width // HEAD_WIDTH, key_pos.shape[1]
    whole = lambda a: pl.BlockSpec(a.shape, lambda h: (0, 0))
    return pl.pallas_call(
        attend_kernel,
        grid=(heads // 2,),
        in_specs=[
            pl.BlockSpec((rows, 2 * HEAD_WIDTH), lambda h: (0, h)),
            whole(keys),
            whole(values),
            whole(kv_other),
            whole(key_pos),
            whole(limit),
        ],
        out_specs=pl.BlockSpec((rows, 2 * HEAD_WIDTH), lambda h: (0, h)),
        out_shape=jax.ShapeDtypeStruct((rows, width), jnp.bfloat16),
        scratch_shapes=[pltpu.VMEM((rows, count), jnp.float32)],
        compiler_params=pltpu.CompilerParams(vmem_limit_bytes=32 << 20),
        cost_estimate=pl.CostEstimate(
            flops=4 * rows * width * count,
            bytes_accessed=4 * rows * width + 4 * count * HEAD_WIDTH,
            transcendentals=rows * heads * count,
        ),
    )(queries, keys, values, kv_other, key_pos, limit)


def project_kernel(a_ref, w_ref, out_ref):
    rows = out_ref.shape[2]
    block = jnp.concatenate([w_ref[j] for j in range(w_ref.shape[0])], axis=1)
    part = jnp.dot(a_ref[...], block, preferred_element_type=jnp.float32).astype(jnp.bfloat16)
    for c in range(out_ref.shape[1]):
        out_ref[0, c] = part[c * rows : (c + 1) * rows]


def project(both, weights, nx):
    chips, depth, wide = weights.shape
    rows, per = both.shape[0] // 2, chips // nx
    return pl.pallas_call(
        project_kernel,
        grid=(nx,),
        in_specs=[
            pl.BlockSpec(both.shape, lambda h: (0, 0)),
            pl.BlockSpec((per, depth, wide), lambda h: (h, 0, 0)),
        ],
        out_specs=pl.BlockSpec((1, 2, rows, per * wide), lambda h: (h, 0, 0, 0)),
        out_shape=jax.ShapeDtypeStruct((nx, 2, rows, per * wide), jnp.bfloat16),
        compiler_params=pltpu.CompilerParams(vmem_limit_bytes=121 << 19),
        cost_estimate=pl.CostEstimate(
            flops=4 * rows * depth * wide * chips,
            bytes_accessed=2 * weights.size,
            transcendentals=0,
        ),
    )(both, weights)


def add_kernel(parts_ref, residual_ref, hidden_ref, square_ref):
    shares, rows, columns = parts_ref.shape
    per = columns // HEAD_WIDTH
    squares = []
    for j in range(per):
        for c in range(2):
            span = slice((2 * j + c) * HEAD_WIDTH, (2 * j + c + 1) * HEAD_WIDTH)
            total = parts_ref[c, :, j * HEAD_WIDTH : (j + 1) * HEAD_WIDTH].astype(jnp.float32)
            for s in range(2 + c, shares, 2):
                total += parts_ref[s, :, j * HEAD_WIDTH : (j + 1) * HEAD_WIDTH].astype(jnp.float32)
            hidden = (residual_ref[:, span].astype(jnp.float32) + total).astype(jnp.bfloat16)
            hidden_ref[:, span] = hidden
            wide = hidden.astype(jnp.float32)
            squares.append(wide * wide)
    copies = square_ref.shape[0]
    square_ref[...] = lax.dot_general(
        jnp.ones((copies, HEAD_WIDTH), jnp.float32),
        sum(squares),
        (((1,), (1,)), ((), ())),
        precision=lax.Precision.HIGHEST,
        preferred_element_type=jnp.float32,
    )


def add_residual(parts, residual, nx):
    shape = residual.shape
    return pl.pallas_call(
        add_kernel,
        in_specs=[VMEM, VMEM],
        out_specs=(VMEM, VMEM),
        out_shape=(
            jax.ShapeDtypeStruct(shape, jnp.bfloat16),
            jax.ShapeDtypeStruct((nx, shape[0]), jnp.float32),
        ),
        compiler_params=pltpu.CompilerParams(vmem_limit_bytes=8 << 20),
        cost_estimate=pl.CostEstimate(
            flops=2 * parts.size, bytes_accessed=2 * parts.size, transcendentals=0
        ),
    )(parts, residual)


def norm_kernel(features, square_ref, hidden_ref, gain_ref, out_ref):
    total = lax.dot_general(
        square_ref[...],
        jnp.ones((square_ref.shape[0], HEAD_WIDTH), jnp.float32),
        (((0,), (0,)), ((), ())),
        precision=lax.Precision.HIGHEST,
        preferred_element_type=jnp.float32,
    )
    factor = lax.rsqrt(total / features + 1e-06)
    for at in range(0, hidden_ref.shape[1], HEAD_WIDTH):
        span = slice(at, at + HEAD_WIDTH)
        wide = hidden_ref[:, span].astype(jnp.float32)
        out_ref[:, span] = (wide * factor * gain_ref[:, span]).astype(jnp.bfloat16)


def normalise(squares, hidden, gain, features):
    return pl.pallas_call(
        functools.partial(norm_kernel, features),
        in_specs=[VMEM, VMEM, VMEM],
        out_specs=VMEM,
        out_shape=jax.ShapeDtypeStruct(hidden.shape, jnp.bfloat16),
        compiler_params=pltpu.CompilerParams(vmem_limit_bytes=8 << 20),
        cost_estimate=pl.CostEstimate(
            flops=4 * hidden.size, bytes_accessed=4 * hidden.size, transcendentals=0
        ),
    )(squares, hidden, gain[None, :])


def shards(queries, keys, values, half_order, frame_lengths, out_proj, residual_in, norm_gain):
    tok_rows = queries.shape[0]
    half_rows = tok_rows // 2
    chips, nx = lax.axis_size("seq"), lax.axis_size("heads")
    z, core = lax.axis_index("seq"), lax.axis_index("sub")
    features = residual_in.shape[1] * nx

    weights = lax.all_gather(out_proj, "seq")
    k_own = lax.all_gather(keys, "seq", tiled=True)
    v_own = lax.all_gather(values, "seq", tiled=True)
    kv_other = swapped(jnp.concatenate([k_own, v_own], axis=0))

    inner = jnp.arange(half_rows, dtype=jnp.int32)
    table = (half_order[:, None] * half_rows + inner[None, :]).reshape(chips, 2, tok_rows)
    of_core = [table[:, 0].reshape(1, -1), table[:, 1].reshape(1, -1)]
    key_pos = jnp.where(
        core == 0,
        jnp.concatenate(of_core, axis=1),
        jnp.concatenate(of_core[::-1], axis=1),
    )
    chosen = (jnp.arange(2 * chips, dtype=jnp.int32) == 2 * z + core)[:, None]
    query_pos = jnp.sum(jnp.where(chosen, table.reshape(2 * chips, tok_rows), 0), axis=0)
    frame_starts = jnp.cumsum(frame_lengths) - frame_lengths
    limit = jnp.sum(
        jnp.where(frame_starts[None, :] <= query_pos[:, None], frame_lengths[None, :], 0), axis=1
    )[:, None]
    attended = attend(queries, k_own, v_own, kv_other, key_pos, limit)

    both = lax.all_gather(attended, "sub", tiled=True)
    parts = project(both, weights, nx).reshape(2 * nx, tok_rows, -1)
    parts = lax.all_to_all(parts, ("heads", "sub"), 0, 0, tiled=True)
    hidden_state, squares = add_residual(parts, residual_in, nx)
    squares = lax.all_to_all(squares, "heads", 0, 0, tiled=True)
    normed = normalise(squares, hidden_state, norm_gain, features)
    return (attended, hidden_state, normed)


def solution(mesh):
    rows = P(("groups", "seq", "sub"), "heads")
    in_specs = (rows, rows, rows, P("groups"), P("groups"), P("heads", ("seq", "sub")), rows, P("heads"))
    return jax.shard_map(
        shards, mesh=mesh, in_specs=in_specs, out_specs=(rows, rows, rows), check_vma=False
    )
```

```python
import functools
import math

import jax
import jax.numpy as jnp
from jax import lax
from jax.experimental import pallas as pl
from jax.experimental.pallas import tpu as pltpu
from jax.sharding import PartitionSpec as P

HEAD_WIDTH = 128
EXP_SCALE = HEAD_WIDTH ** (-0.5) * math.log2(math.e)
STRETCHES, STEP_HEADS = 8, 4
VMEM = pl.BlockSpec(memory_space=pltpu.VMEM)


def swapped(value):
    return lax.ppermute(value, "sub", [(0, 1), (1, 0)])


def attend_kernel(q_ref, k_ref, v_ref, kv_ref, pos_ref, limit_ref, out_ref, bias_ref):
    own, rows = k_ref.shape[0], q_ref.shape[0]
    heads, half = q_ref.shape[1] // HEAD_WIDTH, STRETCHES // 2
    keys = own // half

    @pl.when(pl.program_id(0) == 0)
    def _():
        bias_ref[...] = jnp.where(pos_ref[...] < limit_ref[...], 0.0, -1e30)

    spans = [slice(i * HEAD_WIDTH, (i + 1) * HEAD_WIDTH) for i in range(heads)]
    parts = [slice(i * rows, (i + 1) * rows) for i in range(heads)]
    q = jnp.concatenate([q_ref[:, span] for span in spans], axis=0)

    def scored(j):
        ref, at = (k_ref, j * keys) if j < half else (kv_ref, (j - half) * keys)
        product = lax.dot_general(
            q, ref[at : at + keys], (((1,), (1,)), ((), ())), preferred_element_type=jnp.float32
        )
        bias = bias_ref[:, j * keys : (j + 1) * keys]
        return [product[part] + bias for part in parts]

    scores = scored(0)
    top, total, result = [None] * heads, [None] * heads, [None] * heads
    for j in range(STRETCHES):
        coming = scored(j + 1) if j + 1 < STRETCHES else None
        ref, at = (v_ref, j * keys) if j < half else (kv_ref, own + (j - half) * keys)
        weights, fades = [], []
        for i in range(heads):
            peak = jnp.max(scores[i], axis=-1, keepdims=True) * EXP_SCALE
            if j:
                peak = jnp.maximum(peak, top[i])
            weight = jnp.exp2(scores[i] * EXP_SCALE - peak)
            mass = jnp.sum(weight, axis=-1, keepdims=True)
            if j:
                fades.append(jnp.exp2(top[i] - peak))
                mass += total[i] * fades[i]
            top[i], total[i] = peak, mass
            weights.append(weight.astype(jnp.bfloat16))
        product = jnp.dot(
            jnp.concatenate(weights, axis=0),
            ref[at : at + keys],
            preferred_element_type=jnp.float32,
        )
        for i in range(heads):
            result[i] = product[parts[i]] + (result[i] * fades[i] if j else 0.0)
        scores = coming
    for i in range(heads):
        out_ref[:, spans[i]] = (result[i] / total[i]).astype(out_ref.dtype)


def attend(queries, keys, values, kv_other, key_pos, limit):
    rows, width = queries.shape
    heads, count = width // HEAD_WIDTH, key_pos.shape[1]
    wide = STEP_HEADS * HEAD_WIDTH
    whole = lambda a: pl.BlockSpec(a.shape, lambda h: (0, 0))
    return pl.pallas_call(
        attend_kernel,
        grid=(width // wide,),
        in_specs=[
            pl.BlockSpec((rows, wide), lambda h: (0, h)),
            whole(keys),
            whole(values),
            whole(kv_other),
            whole(key_pos),
            whole(limit),
        ],
        out_specs=pl.BlockSpec((rows, wide), lambda h: (0, h)),
        out_shape=jax.ShapeDtypeStruct((rows, width), jnp.bfloat16),
        scratch_shapes=[pltpu.VMEM((rows, count), jnp.float32)],
        compiler_params=pltpu.CompilerParams(vmem_limit_bytes=32 << 20),
        cost_estimate=pl.CostEstimate(
            flops=4 * rows * width * count,
            bytes_accessed=4 * rows * width + 4 * count * HEAD_WIDTH,
            transcendentals=rows * heads * count,
        ),
    )(queries, keys, values, kv_other, key_pos, limit)


def project_kernel(a_ref, w_ref, out_ref):
    rows = out_ref.shape[2]
    per = w_ref.shape[0] // out_ref.shape[0]
    for h in range(out_ref.shape[0]):
        block = jnp.concatenate([w_ref[per * h + j] for j in range(per)], axis=1)
        part = jnp.dot(a_ref[...], block, preferred_element_type=jnp.float32).astype(jnp.bfloat16)
        for c in range(2):
            out_ref[h, c] = part[c * rows : (c + 1) * rows]


def project(both, weights, nx):
    chips, depth, wide = weights.shape
    rows, per, steps = both.shape[0] // 2, chips // nx, 2
    return pl.pallas_call(
        project_kernel,
        grid=(steps,),
        in_specs=[
            pl.BlockSpec(both.shape, lambda h: (0, 0)),
            pl.BlockSpec((chips // steps, depth, wide), lambda h: (h, 0, 0)),
        ],
        out_specs=pl.BlockSpec((nx // steps, 2, rows, per * wide), lambda h: (h, 0, 0, 0)),
        out_shape=jax.ShapeDtypeStruct((nx, 2, rows, per * wide), jnp.bfloat16),
        compiler_params=pltpu.CompilerParams(vmem_limit_bytes=52 << 20),
        cost_estimate=pl.CostEstimate(
            flops=4 * rows * depth * wide * chips,
            bytes_accessed=2 * weights.size,
            transcendentals=0,
        ),
    )(both, weights)


def add_kernel(parts_ref, residual_ref, hidden_ref, square_ref):
    shares, rows, columns = parts_ref.shape
    squares = []
    for j in range(columns // HEAD_WIDTH):
        at = slice(j * HEAD_WIDTH, (j + 1) * HEAD_WIDTH)
        for c in range(2):
            span = slice((2 * j + c) * HEAD_WIDTH, (2 * j + c + 1) * HEAD_WIDTH)
            total = parts_ref[c, :, at].astype(jnp.float32)
            for s in range(2 + c, shares, 2):
                total += parts_ref[s, :, at].astype(jnp.float32)
            hidden = (residual_ref[:, span].astype(jnp.float32) + total).astype(jnp.bfloat16)
            hidden_ref[:, span] = hidden
            wide = hidden.astype(jnp.float32)
            squares.append(wide * wide)
    copies = square_ref.shape[0]
    square_ref[...] = lax.dot_general(
        jnp.ones((copies, HEAD_WIDTH), jnp.float32),
        sum(squares),
        (((1,), (1,)), ((), ())),
        precision=lax.Precision.HIGHEST,
        preferred_element_type=jnp.float32,
    )


def add_residual(parts, residual, nx):
    shape = residual.shape
    return pl.pallas_call(
        add_kernel,
        in_specs=[VMEM, VMEM],
        out_specs=(VMEM, VMEM),
        out_shape=(
            jax.ShapeDtypeStruct(shape, jnp.bfloat16),
            jax.ShapeDtypeStruct((nx, shape[0]), jnp.float32),
        ),
        compiler_params=pltpu.CompilerParams(vmem_limit_bytes=8 << 20),
        cost_estimate=pl.CostEstimate(
            flops=2 * parts.size, bytes_accessed=2 * parts.size, transcendentals=0
        ),
    )(parts, residual)


def norm_kernel(features, square_ref, hidden_ref, gain_ref, out_ref):
    total = lax.dot_general(
        square_ref[...],
        jnp.ones((square_ref.shape[0], HEAD_WIDTH), jnp.float32),
        (((0,), (0,)), ((), ())),
        precision=lax.Precision.HIGHEST,
        preferred_element_type=jnp.float32,
    )
    factor = lax.rsqrt(total / features + 1e-06)
    for at in range(0, hidden_ref.shape[1], HEAD_WIDTH):
        span = slice(at, at + HEAD_WIDTH)
        wide = hidden_ref[:, span].astype(jnp.float32)
        out_ref[:, span] = (wide * factor * gain_ref[:, span]).astype(jnp.bfloat16)


def normalise(squares, hidden, gain, features):
    return pl.pallas_call(
        functools.partial(norm_kernel, features),
        in_specs=[VMEM, VMEM, VMEM],
        out_specs=VMEM,
        out_shape=jax.ShapeDtypeStruct(hidden.shape, jnp.bfloat16),
        compiler_params=pltpu.CompilerParams(vmem_limit_bytes=8 << 20),
        cost_estimate=pl.CostEstimate(
            flops=4 * hidden.size, bytes_accessed=4 * hidden.size, transcendentals=0
        ),
    )(squares, hidden, gain[None, :])


def shards(queries, keys, values, half_order, frame_lengths, out_proj, residual_in, norm_gain):
    tok_rows = queries.shape[0]
    half_rows = tok_rows // 2
    chips, nx = lax.axis_size("seq"), lax.axis_size("heads")
    z, core = lax.axis_index("seq"), lax.axis_index("sub")
    features = residual_in.shape[1] * nx

    weights = lax.all_gather(out_proj, "seq")
    k_own = lax.all_gather(keys, "seq", tiled=True)
    v_own = lax.all_gather(values, "seq", tiled=True)
    kv_other = swapped(jnp.concatenate([k_own, v_own], axis=0))

    inner = jnp.arange(half_rows, dtype=jnp.int32)
    table = (half_order[:, None] * half_rows + inner[None, :]).reshape(chips, 2, tok_rows)
    of_core = [table[:, 0].reshape(1, -1), table[:, 1].reshape(1, -1)]
    key_pos = jnp.where(
        core == 0,
        jnp.concatenate(of_core, axis=1),
        jnp.concatenate(of_core[::-1], axis=1),
    )
    chosen = (jnp.arange(2 * chips, dtype=jnp.int32) == 2 * z + core)[:, None]
    query_pos = jnp.sum(jnp.where(chosen, table.reshape(2 * chips, tok_rows), 0), axis=0)
    frame_starts = jnp.cumsum(frame_lengths) - frame_lengths
    limit = jnp.sum(
        jnp.where(frame_starts[None, :] <= query_pos[:, None], frame_lengths[None, :], 0), axis=1
    )[:, None]
    attended = attend(queries, k_own, v_own, kv_other, key_pos, limit)

    both = lax.all_gather(attended, "sub", tiled=True)
    parts = project(both, weights, nx).reshape(2 * nx, tok_rows, -1)
    parts = lax.all_to_all(parts, ("heads", "sub"), 0, 0, tiled=True)
    hidden_state, squares = add_residual(parts, residual_in, nx)
    squares = lax.all_to_all(squares, "heads", 0, 0, tiled=True)
    normed = normalise(squares, hidden_state, norm_gain, features)
    return (attended, hidden_state, normed)


def solution(mesh):
    rows = P(("groups", "seq", "sub"), "heads")
    in_specs = (rows, rows, rows, P("groups"), P("groups"), P("heads", ("seq", "sub")), rows, P("heads"))
    return jax.shard_map(
        shards, mesh=mesh, in_specs=in_specs, out_specs=(rows, rows, rows), check_vma=False
    )
```

```python
import functools
import math

import jax
import jax.numpy as jnp
from jax import lax
from jax.experimental import pallas as pl
from jax.experimental.pallas import tpu as pltpu
from jax.sharding import PartitionSpec as P

HEAD_WIDTH = 128
EXP_SCALE = HEAD_WIDTH ** (-0.5) * math.log2(math.e)
STRETCHES, STEP_HEADS = 4, 4
VMEM = pl.BlockSpec(memory_space=pltpu.VMEM)


def swapped(value):
    return lax.ppermute(value, "sub", [(0, 1), (1, 0)])


def attend_kernel(first, q_ref, k_ref, v_ref, pos_ref, limit_ref, *refs):
    if first:
        top_ref, total_ref, result_ref, bias_ref = refs
    else:
        top_in, total_in, result_in, out_ref, bias_ref = refs
    rows, width = q_ref.shape
    keys = k_ref.shape[0] // STRETCHES
    bias_ref[...] = jnp.where(pos_ref[...] < limit_ref[...], 0.0, -1e30)
    parts = [slice(i * rows, (i + 1) * rows) for i in range(STEP_HEADS)]

    for group in range(0, width // HEAD_WIDTH, STEP_HEADS):
        spans = [
            slice(i * HEAD_WIDTH, (i + 1) * HEAD_WIDTH) for i in range(group, group + STEP_HEADS)
        ]
        q = jnp.concatenate([q_ref[:, span] for span in spans], axis=0)

        def scored(j):
            product = lax.dot_general(
                q,
                k_ref[j * keys : (j + 1) * keys],
                (((1,), (1,)), ((), ())),
                preferred_element_type=jnp.float32,
            )
            bias = bias_ref[:, j * keys : (j + 1) * keys]
            return [product[part] + bias for part in parts]

        scores = scored(0)
        if first:
            top, total, result = ([None] * STEP_HEADS for _ in range(3))
        else:
            top = [top_in[:, span][:, :1] for span in spans]
            total = [total_in[:, span][:, :1] for span in spans]
            result = [result_in[:, span] for span in spans]
        for j in range(STRETCHES):
            coming = scored(j + 1) if j + 1 < STRETCHES else None
            fresh = first and j == 0
            weights, fades = [], []
            for i in range(STEP_HEADS):
                peak = jnp.max(scores[i], axis=-1, keepdims=True) * EXP_SCALE
                if not fresh:
                    peak = jnp.maximum(peak, top[i])
                weight = jnp.exp2(scores[i] * EXP_SCALE - peak)
                mass = jnp.sum(weight, axis=-1, keepdims=True)
                if not fresh:
                    fades.append(jnp.exp2(top[i] - peak))
                    mass += total[i] * fades[i]
                top[i], total[i] = peak, mass
                weights.append(weight.astype(jnp.bfloat16))
            product = jnp.dot(
                jnp.concatenate(weights, axis=0),
                v_ref[j * keys : (j + 1) * keys],
                preferred_element_type=jnp.float32,
            )
            for i in range(STEP_HEADS):
                result[i] = product[parts[i]] + (0.0 if fresh else result[i] * fades[i])
            scores = coming
        for i, span in enumerate(spans):
            if first:
                top_ref[:, span] = jnp.broadcast_to(top[i], (rows, HEAD_WIDTH))
                total_ref[:, span] = jnp.broadcast_to(total[i], (rows, HEAD_WIDTH))
                result_ref[:, span] = result[i]
            else:
                out_ref[:, span] = (result[i] / total[i]).astype(out_ref.dtype)


def attend(queries, keys, values, key_pos, limit, state=()):
    rows, width = queries.shape
    count = keys.shape[0]
    running = jax.ShapeDtypeStruct((rows, width), jnp.float32)
    return pl.pallas_call(
        functools.partial(attend_kernel, not state),
        in_specs=[VMEM] * (5 + len(state)),
        out_specs=VMEM if state else (VMEM,) * 3,
        out_shape=jax.ShapeDtypeStruct((rows, width), jnp.bfloat16) if state else (running,) * 3,
        scratch_shapes=[pltpu.VMEM((rows, count), jnp.float32)],
        compiler_params=pltpu.CompilerParams(vmem_limit_bytes=32 << 20),
        cost_estimate=pl.CostEstimate(
            flops=4 * rows * width * count,
            bytes_accessed=4 * rows * width + 4 * count * HEAD_WIDTH,
            transcendentals=rows * count * width // HEAD_WIDTH,
        ),
    )(queries, keys, values, key_pos, limit, *state)


def project_kernel(a_ref, w_ref, out_ref):
    rows = out_ref.shape[2]
    per = w_ref.shape[0] // out_ref.shape[0]
    for h in range(out_ref.shape[0]):
        block = jnp.concatenate([w_ref[per * h + j] for j in range(per)], axis=1)
        part = jnp.dot(a_ref[...], block, preferred_element_type=jnp.float32).astype(jnp.bfloat16)
        for c in range(2):
            out_ref[h, c] = part[c * rows : (c + 1) * rows]


def project(both, weights, nx):
    chips, depth, wide = weights.shape
    rows, per, steps = both.shape[0] // 2, chips // nx, 2
    return pl.pallas_call(
        project_kernel,
        grid=(steps,),
        in_specs=[
            pl.BlockSpec(both.shape, lambda h: (0, 0)),
            pl.BlockSpec((chips // steps, depth, wide), lambda h: (h, 0, 0)),
        ],
        out_specs=pl.BlockSpec((nx // steps, 2, rows, per * wide), lambda h: (h, 0, 0, 0)),
        out_shape=jax.ShapeDtypeStruct((nx, 2, rows, per * wide), jnp.bfloat16),
        compiler_params=pltpu.CompilerParams(vmem_limit_bytes=52 << 20),
        cost_estimate=pl.CostEstimate(
            flops=4 * rows * depth * wide * chips,
            bytes_accessed=2 * weights.size,
            transcendentals=0,
        ),
    )(both, weights)


def add_kernel(parts_ref, residual_ref, hidden_ref, twin_ref, square_ref):
    shares, rows, columns = parts_ref.shape
    squares = []
    for j in range(columns // HEAD_WIDTH):
        at = slice(j * HEAD_WIDTH, (j + 1) * HEAD_WIDTH)
        for c in range(2):
            span = slice((2 * j + c) * HEAD_WIDTH, (2 * j + c + 1) * HEAD_WIDTH)
            total = parts_ref[c, :, at].astype(jnp.float32)
            for s in range(2 + c, shares, 2):
                total += parts_ref[s, :, at].astype(jnp.float32)
            hidden = (residual_ref[:, span].astype(jnp.float32) + total).astype(jnp.bfloat16)
            hidden_ref[:, span] = hidden
            twin_ref[:, span] = hidden
            wide = hidden.astype(jnp.float32)
            squares.append(wide * wide)
    copies = square_ref.shape[0]
    square_ref[...] = lax.dot_general(
        jnp.ones((copies, HEAD_WIDTH), jnp.float32),
        sum(squares),
        (((1,), (1,)), ((), ())),
        precision=lax.Precision.HIGHEST,
        preferred_element_type=jnp.float32,
    )


def add_residual(parts, residual, nx):
    shape = residual.shape
    return pl.pallas_call(
        add_kernel,
        in_specs=[VMEM, VMEM],
        out_specs=(VMEM, VMEM, VMEM),
        out_shape=(
            jax.ShapeDtypeStruct(shape, jnp.bfloat16),
            jax.ShapeDtypeStruct(shape, jnp.bfloat16),
            jax.ShapeDtypeStruct((nx, shape[0]), jnp.float32),
        ),
        compiler_params=pltpu.CompilerParams(vmem_limit_bytes=8 << 20),
        cost_estimate=pl.CostEstimate(
            flops=2 * parts.size, bytes_accessed=2 * parts.size, transcendentals=0
        ),
    )(parts, residual)


def norm_kernel(features, square_ref, hidden_ref, gain_ref, out_ref):
    total = lax.dot_general(
        square_ref[...],
        jnp.ones((square_ref.shape[0], HEAD_WIDTH), jnp.float32),
        (((0,), (0,)), ((), ())),
        precision=lax.Precision.HIGHEST,
        preferred_element_type=jnp.float32,
    )
    factor = lax.rsqrt(total / features + 1e-06)
    for at in range(0, hidden_ref.shape[1], HEAD_WIDTH):
        span = slice(at, at + HEAD_WIDTH)
        wide = hidden_ref[:, span].astype(jnp.float32)
        out_ref[:, span] = (wide * factor * gain_ref[:, span]).astype(jnp.bfloat16)


def normalise(squares, hidden, gain, features):
    return pl.pallas_call(
        functools.partial(norm_kernel, features),
        in_specs=[VMEM, VMEM, VMEM],
        out_specs=VMEM,
        out_shape=jax.ShapeDtypeStruct(hidden.shape, jnp.bfloat16),
        compiler_params=pltpu.CompilerParams(vmem_limit_bytes=8 << 20),
        cost_estimate=pl.CostEstimate(
            flops=4 * hidden.size, bytes_accessed=4 * hidden.size, transcendentals=0
        ),
    )(squares, hidden, gain[None, :])


def shards(queries, keys, values, half_order, frame_lengths, out_proj, residual_in, norm_gain):
    tok_rows = queries.shape[0]
    half_rows = tok_rows // 2
    chips, nx = lax.axis_size("seq"), lax.axis_size("heads")
    z, core = lax.axis_index("seq"), lax.axis_index("sub")
    features = residual_in.shape[1] * nx

    weights = lax.all_gather(out_proj, "seq")
    k_own = lax.all_gather(keys, "seq", tiled=True)
    v_own = lax.all_gather(values, "seq", tiled=True)
    kv_other = swapped(jnp.concatenate([k_own, v_own], axis=0))

    inner = jnp.arange(half_rows, dtype=jnp.int32)
    table = (half_order[:, None] * half_rows + inner[None, :]).reshape(chips, 2, tok_rows)
    of_core = [table[:, 0].reshape(1, -1), table[:, 1].reshape(1, -1)]
    pos_own = jnp.where(core == 0, of_core[0], of_core[1])
    pos_other = jnp.where(core == 0, of_core[1], of_core[0])
    chosen = (jnp.arange(2 * chips, dtype=jnp.int32) == 2 * z + core)[:, None]
    query_pos = jnp.sum(jnp.where(chosen, table.reshape(2 * chips, tok_rows), 0), axis=0)
    frame_starts = jnp.cumsum(frame_lengths) - frame_lengths
    limit = jnp.sum(
        jnp.where(frame_starts[None, :] <= query_pos[:, None], frame_lengths[None, :], 0), axis=1
    )[:, None]
    state = attend(queries, k_own, v_own, pos_own, limit)
    k_other, v_other = kv_other[: k_own.shape[0]], kv_other[k_own.shape[0] :]
    attended = attend(queries, k_other, v_other, pos_other, limit, state)

    both = lax.all_gather(attended, "sub", tiled=True)
    parts = project(both, weights, nx).reshape(2 * nx, tok_rows, -1)
    parts = lax.all_to_all(parts, ("heads", "sub"), 0, 0, tiled=True)
    hidden_state, twin, squares = add_residual(parts, residual_in, nx)
    squares = lax.all_to_all(squares, "heads", 0, 0, tiled=True)
    normed = normalise(squares, twin, norm_gain, features)
    return (attended, hidden_state, normed)


def solution(mesh):
    rows = P(("groups", "seq", "sub"), "heads")
    in_specs = (rows, rows, rows, P("groups"), P("groups"), P("heads", ("seq", "sub")), rows, P("heads"))
    return jax.shard_map(
        shards, mesh=mesh, in_specs=in_specs, out_specs=(rows, rows, rows), check_vma=False
    )
```

```python
import functools
import math

import jax
import jax.numpy as jnp
from jax import lax
from jax.experimental import pallas as pl
from jax.experimental.pallas import tpu as pltpu
from jax.sharding import PartitionSpec as P

HEAD_WIDTH = 128
EXP_SCALE = HEAD_WIDTH ** (-0.5) * math.log2(math.e)
STRETCHES, STEP_HEADS = 4, 4
VMEM = pl.BlockSpec(memory_space=pltpu.VMEM)


def swapped(value):
    return lax.ppermute(value, "sub", [(0, 1), (1, 0)])


def attend_kernel(first, q_ref, k_ref, v_ref, pos_ref, limit_ref, *refs):
    if first:
        top_ref, total_ref, result_ref, bias_ref = refs
    else:
        top_in, total_in, result_in, out_ref, bias_ref = refs
    rows, width = q_ref.shape
    keys = k_ref.shape[0] // STRETCHES
    bias_ref[...] = jnp.where(pos_ref[...] < limit_ref[...], 0.0, -1e30)
    parts = [slice(i * rows, (i + 1) * rows) for i in range(STEP_HEADS)]

    for group in range(0, width // HEAD_WIDTH, STEP_HEADS):
        spans = [
            slice(i * HEAD_WIDTH, (i + 1) * HEAD_WIDTH) for i in range(group, group + STEP_HEADS)
        ]
        q = jnp.concatenate([q_ref[:, span] for span in spans], axis=0)

        def scored(j):
            product = lax.dot_general(
                q,
                k_ref[j * keys : (j + 1) * keys],
                (((1,), (1,)), ((), ())),
                preferred_element_type=jnp.float32,
            )
            bias = bias_ref[:, j * keys : (j + 1) * keys]
            return [product[part] + bias for part in parts]

        scores = scored(0)
        if first:
            top, total, result = ([None] * STEP_HEADS for _ in range(3))
        else:
            top = [jnp.max(top_in[:, span], axis=-1, keepdims=True) for span in spans]
            total = [jnp.max(total_in[:, span], axis=-1, keepdims=True) for span in spans]
            result = [result_in[:, span] for span in spans]
        for j in range(STRETCHES):
            coming = scored(j + 1) if j + 1 < STRETCHES else None
            fresh = first and j == 0
            weights, fades = [], []
            for i in range(STEP_HEADS):
                peak = jnp.max(scores[i], axis=-1, keepdims=True) * EXP_SCALE
                if not fresh:
                    peak = jnp.maximum(peak, top[i])
                weight = jnp.exp2(scores[i] * EXP_SCALE - peak)
                mass = jnp.sum(weight, axis=-1, keepdims=True)
                if not fresh:
                    fades.append(jnp.exp2(top[i] - peak))
                    mass += total[i] * fades[i]
                top[i], total[i] = peak, mass
                weights.append(weight.astype(jnp.bfloat16))
            product = jnp.dot(
                jnp.concatenate(weights, axis=0),
                v_ref[j * keys : (j + 1) * keys],
                preferred_element_type=jnp.float32,
            )
            for i in range(STEP_HEADS):
                result[i] = product[parts[i]] + (0.0 if fresh else result[i] * fades[i])
            scores = coming
        for i, span in enumerate(spans):
            if first:
                top_ref[:, span] = jnp.broadcast_to(top[i], (rows, HEAD_WIDTH))
                total_ref[:, span] = jnp.broadcast_to(total[i], (rows, HEAD_WIDTH))
                result_ref[:, span] = result[i]
            else:
                out_ref[:, span] = (result[i] / total[i]).astype(out_ref.dtype)


def attend(queries, keys, values, key_pos, limit, state=()):
    rows, width = queries.shape
    count = keys.shape[0]
    running = jax.ShapeDtypeStruct((rows, width), jnp.float32)
    return pl.pallas_call(
        functools.partial(attend_kernel, not state),
        in_specs=[VMEM] * (5 + len(state)),
        out_specs=VMEM if state else (VMEM,) * 3,
        out_shape=jax.ShapeDtypeStruct((rows, width), jnp.bfloat16) if state else (running,) * 3,
        scratch_shapes=[pltpu.VMEM((rows, count), jnp.float32)],
        compiler_params=pltpu.CompilerParams(vmem_limit_bytes=32 << 20),
        cost_estimate=pl.CostEstimate(
            flops=4 * rows * width * count,
            bytes_accessed=4 * rows * width + 4 * count * HEAD_WIDTH,
            transcendentals=rows * count * width // HEAD_WIDTH,
        ),
    )(queries, keys, values, key_pos, limit, *state)


def project_kernel(a_ref, w_ref, out_ref):
    rows = out_ref.shape[2]
    per = w_ref.shape[0] // out_ref.shape[0]
    for h in range(out_ref.shape[0]):
        block = jnp.concatenate([w_ref[per * h + j] for j in range(per)], axis=1)
        part = jnp.dot(a_ref[...], block, preferred_element_type=jnp.float32).astype(jnp.bfloat16)
        for c in range(2):
            out_ref[h, c] = part[c * rows : (c + 1) * rows]


def project(both, weights, nx):
    chips, depth, wide = weights.shape
    rows, per, steps = both.shape[0] // 2, chips // nx, 2
    return pl.pallas_call(
        project_kernel,
        grid=(steps,),
        in_specs=[
            pl.BlockSpec(both.shape, lambda h: (0, 0)),
            pl.BlockSpec((chips // steps, depth, wide), lambda h: (h, 0, 0)),
        ],
        out_specs=pl.BlockSpec((nx // steps, 2, rows, per * wide), lambda h: (h, 0, 0, 0)),
        out_shape=jax.ShapeDtypeStruct((nx, 2, rows, per * wide), jnp.bfloat16),
        compiler_params=pltpu.CompilerParams(vmem_limit_bytes=52 << 20),
        cost_estimate=pl.CostEstimate(
            flops=4 * rows * depth * wide * chips,
            bytes_accessed=2 * weights.size,
            transcendentals=0,
        ),
    )(both, weights)


def add_kernel(parts_ref, residual_ref, hidden_ref, twin_ref, square_ref):
    shares, rows, columns = parts_ref.shape
    squares = []
    for j in range(columns // HEAD_WIDTH):
        at = slice(j * HEAD_WIDTH, (j + 1) * HEAD_WIDTH)
        for c in range(2):
            span = slice((2 * j + c) * HEAD_WIDTH, (2 * j + c + 1) * HEAD_WIDTH)
            total = parts_ref[c, :, at].astype(jnp.float32)
            for s in range(2 + c, shares, 2):
                total += parts_ref[s, :, at].astype(jnp.float32)
            hidden = (residual_ref[:, span].astype(jnp.float32) + total).astype(jnp.bfloat16)
            hidden_ref[:, span] = hidden
            twin_ref[:, span] = hidden
            wide = hidden.astype(jnp.float32)
            squares.append(wide * wide)
    copies = square_ref.shape[0]
    square_ref[...] = lax.dot_general(
        jnp.ones((copies, HEAD_WIDTH), jnp.float32),
        sum(squares),
        (((1,), (1,)), ((), ())),
        precision=lax.Precision.HIGHEST,
        preferred_element_type=jnp.float32,
    )


def add_residual(parts, residual, nx):
    shape = residual.shape
    return pl.pallas_call(
        add_kernel,
        in_specs=[VMEM, VMEM],
        out_specs=(VMEM, VMEM, VMEM),
        out_shape=(
            jax.ShapeDtypeStruct(shape, jnp.bfloat16),
            jax.ShapeDtypeStruct(shape, jnp.bfloat16),
            jax.ShapeDtypeStruct((nx, shape[0]), jnp.float32),
        ),
        compiler_params=pltpu.CompilerParams(vmem_limit_bytes=8 << 20),
        cost_estimate=pl.CostEstimate(
            flops=2 * parts.size, bytes_accessed=2 * parts.size, transcendentals=0
        ),
    )(parts, residual)


def norm_kernel(features, square_ref, hidden_ref, gain_ref, out_ref):
    total = lax.dot_general(
        square_ref[...],
        jnp.ones((square_ref.shape[0], HEAD_WIDTH), jnp.float32),
        (((0,), (0,)), ((), ())),
        precision=lax.Precision.HIGHEST,
        preferred_element_type=jnp.float32,
    )
    factor = lax.rsqrt(total / features + 1e-06)
    for at in range(0, hidden_ref.shape[1], HEAD_WIDTH):
        span = slice(at, at + HEAD_WIDTH)
        wide = hidden_ref[:, span].astype(jnp.float32)
        out_ref[:, span] = (wide * factor * gain_ref[:, span]).astype(jnp.bfloat16)


def normalise(squares, hidden, gain, features):
    return pl.pallas_call(
        functools.partial(norm_kernel, features),
        in_specs=[VMEM, VMEM, VMEM],
        out_specs=VMEM,
        out_shape=jax.ShapeDtypeStruct(hidden.shape, jnp.bfloat16),
        compiler_params=pltpu.CompilerParams(vmem_limit_bytes=8 << 20),
        cost_estimate=pl.CostEstimate(
            flops=4 * hidden.size, bytes_accessed=4 * hidden.size, transcendentals=0
        ),
    )(squares, hidden, gain[None, :])


def shards(queries, keys, values, half_order, frame_lengths, out_proj, residual_in, norm_gain):
    tok_rows = queries.shape[0]
    half_rows = tok_rows // 2
    chips, nx = lax.axis_size("seq"), lax.axis_size("heads")
    z, core = lax.axis_index("seq"), lax.axis_index("sub")
    features = residual_in.shape[1] * nx

    weights = lax.all_gather(out_proj, "seq")
    k_own = lax.all_gather(keys, "seq", tiled=True)
    v_own = lax.all_gather(values, "seq", tiled=True)
    kv_other = swapped(jnp.concatenate([k_own, v_own], axis=0))

    inner = jnp.arange(half_rows, dtype=jnp.int32)
    table = (half_order[:, None] * half_rows + inner[None, :]).reshape(chips, 2, tok_rows)
    of_core = [table[:, 0].reshape(1, -1), table[:, 1].reshape(1, -1)]
    pos_own = jnp.where(core == 0, of_core[0], of_core[1])
    pos_other = jnp.where(core == 0, of_core[1], of_core[0])
    chosen = (jnp.arange(2 * chips, dtype=jnp.int32) == 2 * z + core)[:, None]
    query_pos = jnp.sum(jnp.where(chosen, table.reshape(2 * chips, tok_rows), 0), axis=0)
    frame_starts = jnp.cumsum(frame_lengths) - frame_lengths
    limit = jnp.sum(
        jnp.where(frame_starts[None, :] <= query_pos[:, None], frame_lengths[None, :], 0), axis=1
    )[:, None]
    state = attend(queries, k_own, v_own, pos_own, limit)
    k_other, v_other = kv_other[: k_own.shape[0]], kv_other[k_own.shape[0] :]
    attended = attend(queries, k_other, v_other, pos_other, limit, state)

    both = lax.all_gather(attended, "sub", tiled=True)
    parts = project(both, weights, nx).reshape(2 * nx, tok_rows, -1)
    parts = lax.all_to_all(parts, ("heads", "sub"), 0, 0, tiled=True)
    hidden_state, twin, squares = add_residual(parts, residual_in, nx)
    squares = lax.all_to_all(squares, "heads", 0, 0, tiled=True)
    normed = normalise(squares, twin, norm_gain, features)
    return (attended, hidden_state, normed)


def solution(mesh):
    rows = P(("groups", "seq", "sub"), "heads")
    in_specs = (rows, rows, rows, P("groups"), P("groups"), P("heads", ("seq", "sub")), rows, P("heads"))
    return jax.shard_map(
        shards, mesh=mesh, in_specs=in_specs, out_specs=(rows, rows, rows), check_vma=False
    )
```

```python
import functools
import math

import jax
import jax.numpy as jnp
from jax import lax
from jax.experimental import pallas as pl
from jax.experimental.pallas import tpu as pltpu
from jax.sharding import PartitionSpec as P

HEAD_WIDTH = 128
EXP_SCALE = HEAD_WIDTH ** (-0.5) * math.log2(math.e)
STRETCHES, STEP_HEADS = 4, 4
VMEM = pl.BlockSpec(memory_space=pltpu.VMEM)


def swapped(value):
    return lax.ppermute(value, "sub", [(0, 1), (1, 0)])


def attend_kernel(first, q_ref, k_ref, v_ref, pos_ref, limit_ref, *refs):
    if first:
        top_ref, total_ref, result_ref, bias_ref = refs
    else:
        top_in, total_in, result_in, out_ref, bias_ref = refs
    rows, width = q_ref.shape
    keys = k_ref.shape[0] // STRETCHES
    bias_ref[...] = jnp.where(pos_ref[...] < limit_ref[...], 0.0, -1e30)
    parts = [slice(i * rows, (i + 1) * rows) for i in range(STEP_HEADS)]

    for group in range(0, width // HEAD_WIDTH, STEP_HEADS):
        spans = [
            slice(i * HEAD_WIDTH, (i + 1) * HEAD_WIDTH) for i in range(group, group + STEP_HEADS)
        ]
        q = jnp.concatenate([q_ref[:, span] for span in spans], axis=0)

        def scored(j):
            product = lax.dot_general(
                q,
                k_ref[j * keys : (j + 1) * keys],
                (((1,), (1,)), ((), ())),
                preferred_element_type=jnp.float32,
            )
            bias = bias_ref[:, j * keys : (j + 1) * keys]
            return [product[part] + bias for part in parts]

        scores = scored(0)
        if first:
            top, total, result = ([None] * STEP_HEADS for _ in range(3))
        else:
            top = [jnp.max(top_in[:, span], axis=-1, keepdims=True) for span in spans]
            total = [jnp.max(total_in[:, span], axis=-1, keepdims=True) for span in spans]
            result = [result_in[:, span] for span in spans]
        for j in range(STRETCHES):
            coming = scored(j + 1) if j + 1 < STRETCHES else None
            fresh = first and j == 0
            weights, fades = [], []
            for i in range(STEP_HEADS):
                peak = jnp.max(scores[i], axis=-1, keepdims=True) * EXP_SCALE
                if not fresh:
                    peak = jnp.maximum(peak, top[i])
                weight = jnp.exp2(scores[i] * EXP_SCALE - peak)
                mass = jnp.sum(weight, axis=-1, keepdims=True)
                if not fresh:
                    fades.append(jnp.exp2(top[i] - peak))
                    mass += total[i] * fades[i]
                top[i], total[i] = peak, mass
                weights.append(weight.astype(jnp.bfloat16))
            product = jnp.dot(
                jnp.concatenate(weights, axis=0),
                v_ref[j * keys : (j + 1) * keys],
                preferred_element_type=jnp.float32,
            )
            for i in range(STEP_HEADS):
                result[i] = product[parts[i]] + (0.0 if fresh else result[i] * fades[i])
            scores = coming
        for i, span in enumerate(spans):
            if first:
                top_ref[:, span] = jnp.broadcast_to(top[i], (rows, HEAD_WIDTH))
                total_ref[:, span] = jnp.broadcast_to(total[i], (rows, HEAD_WIDTH))
                result_ref[:, span] = result[i]
            else:
                out_ref[:, span] = (result[i] / total[i]).astype(out_ref.dtype)


def attend(queries, keys, values, key_pos, limit, state=()):
    rows, width = queries.shape
    count = keys.shape[0]
    running = jax.ShapeDtypeStruct((rows, width), jnp.float32)
    return pl.pallas_call(
        functools.partial(attend_kernel, not state),
        in_specs=[VMEM] * (5 + len(state)),
        out_specs=VMEM if state else (VMEM,) * 3,
        out_shape=jax.ShapeDtypeStruct((rows, width), jnp.bfloat16) if state else (running,) * 3,
        scratch_shapes=[pltpu.VMEM((rows, count), jnp.float32)],
        compiler_params=pltpu.CompilerParams(vmem_limit_bytes=32 << 20),
        cost_estimate=pl.CostEstimate(
            flops=4 * rows * width * count,
            bytes_accessed=4 * rows * width + 4 * count * HEAD_WIDTH,
            transcendentals=rows * count * width // HEAD_WIDTH,
        ),
    )(queries, keys, values, key_pos, limit, *state)


def project_kernel(a_ref, w_ref, out_ref):
    rows = out_ref.shape[2]
    per = w_ref.shape[0] // out_ref.shape[0]
    for h in range(out_ref.shape[0]):
        block = jnp.concatenate([w_ref[per * h + j] for j in range(per)], axis=1)
        part = jnp.dot(a_ref[...], block, preferred_element_type=jnp.float32).astype(jnp.bfloat16)
        for c in range(2):
            out_ref[h, c] = part[c * rows : (c + 1) * rows]


def project(both, weights, nx):
    chips, depth, wide = weights.shape
    rows, per, steps = both.shape[0] // 2, chips // nx, 2
    return pl.pallas_call(
        project_kernel,
        grid=(steps,),
        in_specs=[
            pl.BlockSpec(both.shape, lambda h: (0, 0)),
            pl.BlockSpec((chips // steps, depth, wide), lambda h: (h, 0, 0)),
        ],
        out_specs=pl.BlockSpec((nx // steps, 2, rows, per * wide), lambda h: (h, 0, 0, 0)),
        out_shape=jax.ShapeDtypeStruct((nx, 2, rows, per * wide), jnp.bfloat16),
        compiler_params=pltpu.CompilerParams(vmem_limit_bytes=52 << 20),
        cost_estimate=pl.CostEstimate(
            flops=4 * rows * depth * wide * chips,
            bytes_accessed=2 * weights.size,
            transcendentals=0,
        ),
    )(both, weights)


def sum_kernel(parts_ref, out_ref):
    total = parts_ref[0].astype(jnp.float32)
    for s in range(1, parts_ref.shape[0]):
        total += parts_ref[s].astype(jnp.float32)
    out_ref[...] = total


def sum_shares(parts):
    return pl.pallas_call(
        sum_kernel,
        in_specs=[VMEM],
        out_specs=VMEM,
        out_shape=jax.ShapeDtypeStruct(parts.shape[1:], jnp.float32),
        compiler_params=pltpu.CompilerParams(vmem_limit_bytes=8 << 20),
        cost_estimate=pl.CostEstimate(
            flops=2 * parts.size, bytes_accessed=2 * parts.size, transcendentals=0
        ),
    )(parts)


def add_kernel(sums_ref, residual_ref, hidden_ref, twin_ref, square_ref):
    squares = []
    for j in range(sums_ref.shape[2] // HEAD_WIDTH):
        at = slice(j * HEAD_WIDTH, (j + 1) * HEAD_WIDTH)
        for c in range(2):
            span = slice((2 * j + c) * HEAD_WIDTH, (2 * j + c + 1) * HEAD_WIDTH)
            total = residual_ref[:, span].astype(jnp.float32) + sums_ref[c, :, at]
            hidden = total.astype(jnp.bfloat16)
            hidden_ref[:, span] = hidden
            twin_ref[:, span] = hidden
            wide = hidden.astype(jnp.float32)
            squares.append(wide * wide)
    copies = square_ref.shape[0]
    square_ref[...] = lax.dot_general(
        jnp.ones((copies, HEAD_WIDTH), jnp.float32),
        sum(squares),
        (((1,), (1,)), ((), ())),
        precision=lax.Precision.HIGHEST,
        preferred_element_type=jnp.float32,
    )


def add_residual(sums, residual, nx):
    shape = residual.shape
    return pl.pallas_call(
        add_kernel,
        in_specs=[VMEM, VMEM],
        out_specs=(VMEM, VMEM, VMEM),
        out_shape=(
            jax.ShapeDtypeStruct(shape, jnp.bfloat16),
            jax.ShapeDtypeStruct(shape, jnp.bfloat16),
            jax.ShapeDtypeStruct((nx, shape[0]), jnp.float32),
        ),
        compiler_params=pltpu.CompilerParams(vmem_limit_bytes=8 << 20),
        cost_estimate=pl.CostEstimate(
            flops=4 * sums.size, bytes_accessed=4 * sums.size, transcendentals=0
        ),
    )(sums, residual)


def norm_kernel(features, square_ref, hidden_ref, gain_ref, out_ref):
    total = lax.dot_general(
        square_ref[...],
        jnp.ones((square_ref.shape[0], HEAD_WIDTH), jnp.float32),
        (((0,), (0,)), ((), ())),
        precision=lax.Precision.HIGHEST,
        preferred_element_type=jnp.float32,
    )
    factor = lax.rsqrt(total / features + 1e-06)
    for at in range(0, hidden_ref.shape[1], HEAD_WIDTH):
        span = slice(at, at + HEAD_WIDTH)
        wide = hidden_ref[:, span].astype(jnp.float32)
        out_ref[:, span] = (wide * factor * gain_ref[:, span]).astype(jnp.bfloat16)


def normalise(squares, hidden, gain, features):
    return pl.pallas_call(
        functools.partial(norm_kernel, features),
        in_specs=[VMEM, VMEM, VMEM],
        out_specs=VMEM,
        out_shape=jax.ShapeDtypeStruct(hidden.shape, jnp.bfloat16),
        compiler_params=pltpu.CompilerParams(vmem_limit_bytes=8 << 20),
        cost_estimate=pl.CostEstimate(
            flops=4 * hidden.size, bytes_accessed=4 * hidden.size, transcendentals=0
        ),
    )(squares, hidden, gain[None, :])


def shards(queries, keys, values, half_order, frame_lengths, out_proj, residual_in, norm_gain):
    tok_rows = queries.shape[0]
    half_rows = tok_rows // 2
    chips, nx = lax.axis_size("seq"), lax.axis_size("heads")
    z, core = lax.axis_index("seq"), lax.axis_index("sub")
    features = residual_in.shape[1] * nx

    weights = lax.all_gather(out_proj, "seq")
    k_own = lax.all_gather(keys, "seq", tiled=True)
    v_own = lax.all_gather(values, "seq", tiled=True)
    kv_other = swapped(jnp.concatenate([k_own, v_own], axis=0))

    inner = jnp.arange(half_rows, dtype=jnp.int32)
    table = (half_order[:, None] * half_rows + inner[None, :]).reshape(chips, 2, tok_rows)
    of_core = [table[:, 0].reshape(1, -1), table[:, 1].reshape(1, -1)]
    pos_own = jnp.where(core == 0, of_core[0], of_core[1])
    pos_other = jnp.where(core == 0, of_core[1], of_core[0])
    chosen = (jnp.arange(2 * chips, dtype=jnp.int32) == 2 * z + core)[:, None]
    query_pos = jnp.sum(jnp.where(chosen, table.reshape(2 * chips, tok_rows), 0), axis=0)
    frame_starts = jnp.cumsum(frame_lengths) - frame_lengths
    limit = jnp.sum(
        jnp.where(frame_starts[None, :] <= query_pos[:, None], frame_lengths[None, :], 0), axis=1
    )[:, None]
    state = attend(queries, k_own, v_own, pos_own, limit)
    k_other, v_other = kv_other[: k_own.shape[0]], kv_other[k_own.shape[0] :]
    attended = attend(queries, k_other, v_other, pos_other, limit, state)

    both = lax.all_gather(attended, "sub", tiled=True)
    parts = project(both, weights, nx).reshape(nx, 2 * tok_rows, -1)
    sums = sum_shares(lax.all_to_all(parts, "heads", 0, 0, tiled=True))
    sums = lax.all_to_all(sums.reshape(2, tok_rows, -1), "sub", 0, 0, tiled=True)
    hidden_state, twin, squares = add_residual(sums, residual_in, nx)
    squares = lax.all_to_all(squares, "heads", 0, 0, tiled=True)
    normed = normalise(squares, twin, norm_gain, features)
    return (attended, hidden_state, normed)


def solution(mesh):
    rows = P(("groups", "seq", "sub"), "heads")
    in_specs = (rows, rows, rows, P("groups"), P("groups"), P("heads", ("seq", "sub")), rows, P("heads"))
    return jax.shard_map(
        shards, mesh=mesh, in_specs=in_specs, out_specs=(rows, rows, rows), check_vma=False
    )
```
